128 devices in a mesh: dp: 4 (over y_hi, core), seq: 32 (over y_lo, x, z).
Axes of the slice: x: 4, y: 4 (y_hi: 2, y_lo: 2; y = y_hi * 2 + y_lo), z: 4, core: 2. Of those that a mesh axis runs over, the one named last changes fastest.
Arguments:
- queries: bfloat16 [131072, 1024], P(('dp', 'seq')), parts along dimension 0, may hold values from -6 to 6
- keys: bfloat16 [131072, 1024], P(('dp', 'seq')), parts along dimension 0, may hold values from -6 to 6
- values: bfloat16 [131072, 1024], P(('dp', 'seq')), parts along dimension 0, may hold values from -6 to 6
Outputs:
- attended: bfloat16 [131072, 1024], P(('dp', 'seq')), parts along dimension 0
- far_attended: bfloat16 [4096, 1024], P(('dp', 'seq')), parts along dimension 0
The draws below stay inside these ranges and needn't reach their ends.
There are 4 independent parts, one for each index of `dp`. The reference program is written for one: setup_inputs(seed, part) draws one part's arguments, and reference() takes and returns one part's arrays. A program takes and returns all parts, laid end to end along the dimension named above; each array names one. Nothing has to cross between parts.
All inputs are finite; a program needn't handle non-finite values.
Results may differ from the reference program's by a relative error of at most 0.0095.
Values may be sent and summed in bfloat16 or wider, within the bound.
No kernel may reach another device: no remote copies, remote signals or barrier semaphores. Data moves between devices by JAX's collectives and lax.ppermute only.
A program may use at most 192 MiB of HBM per device.

```python
import jax
import jax.numpy as jnp
import numpy as np
from jax import lax

H = 16
HD = 64
TOK_DEV = 1024
MIDDLE_DILATION = 4
OUTER_DILATION = 32
MIDDLE_SEGMENT = 16384
TOKENS = 32768


def draw_queries(key, part):
    drawn = jnp.clip(jax.random.normal(jax.random.fold_in(key, 1), (TOKENS, H, HD), jnp.float32) * 1.5, -6.0, 6.0)
    return drawn.reshape(TOKENS, H * HD).astype(jnp.bfloat16)


def draw_keys(key, part):
    drawn = jnp.clip(jax.random.normal(jax.random.fold_in(key, 2), (TOKENS, H, HD), jnp.float32) * 1.5, -6.0, 6.0)
    return drawn.reshape(TOKENS, H * HD).astype(jnp.bfloat16)


def block_levels(stream_key, shape, cuts, smallest, top_value):
    factor_of, own = 1.0, jax.random.fold_in(stream_key, 6)
    for axis_at, blocks in cuts:
        steps = jnp.exp(jax.random.uniform(jax.random.fold_in(own, axis_at), (blocks,), jnp.float32, smallest / len(cuts), top_value / len(cuts)))
        factor_of = factor_of * jnp.repeat(steps, shape[axis_at] // blocks).reshape([-1 if axis == axis_at else 1 for axis in range(len(shape))])
    return factor_of


def normal_values(key, shape, deviation, most, cuts=(), dtype=jnp.bfloat16):
    values = jax.random.normal(key, shape, jnp.float32) * deviation
    if len(cuts) > 0:
        values = block_levels(key, shape, cuts, -0.22, 0.18) * values
    return jnp.clip(values, min=-most, max=most).astype(dtype)


def setup_inputs(seed: int = 0, part: int = 0) -> dict:
    streams_of = jax.random.split(jax.random.key(seed), 4)
    part_splits = jax.random.split(jax.random.fold_in(streams_of[3], part), 4)
    queries = draw_queries(jax.random.fold_in(jax.random.fold_in(streams_of[3], part), 71), part)
    keys = draw_keys(jax.random.fold_in(jax.random.fold_in(streams_of[3], part), 71), part)
    values = normal_values(part_splits[2], (TOKENS, H * HD), 1.0, 6.0, ((0, 32),))
    return {"queries": queries, "keys": keys, "values": values}


VOID_LEVEL = -1.0e30


def attend_one(query, keys, values):
    factor = query.shape[-1] ** -0.5
    scores = jnp.einsum("qd,kd->qk", query.astype(jnp.float32), keys.astype(jnp.float32)) * factor
    peak = jnp.max(scores, axis=-1, keepdims=True)
    powers = jnp.exp(scores - peak)
    total = jnp.sum(powers, axis=-1, keepdims=True)
    rounded = lax.optimization_barrier(powers.astype(jnp.bfloat16)).astype(jnp.float32)
    mixed = jnp.einsum("qk,kd->qd", rounded, values.astype(jnp.float32)) / total
    return mixed.astype(jnp.bfloat16), peak[:, 0] + jnp.log(total[:, 0])


def attend_per_head(query, keys, values):
    return lax.map(lambda triple: attend_one(triple[0], triple[1], triple[2]), (query, keys, values))


def to_heads(array):
    length = array.shape[0]
    return array.reshape(length, H, HD).transpose(1, 0, 2)


def dilate_tokens(array, rate):
    heads, length, depth = array.shape
    offsets = np.arange(heads) % rate
    return array.reshape(heads, length // rate, rate, depth)[np.arange(heads), :, offsets, :]


def spread_back(mixed, level, rate):
    heads, count, depth = mixed.shape
    chosen = np.arange(rate)[None, :] == (np.arange(heads) % rate)[:, None]
    full_out = (mixed.astype(jnp.float32)[:, :, None, :] * chosen.astype(np.float32)[:, None, :, None]).reshape(heads, count * rate, depth)
    full_level = jnp.where(chosen[:, None, :], level[:, :, None], VOID_LEVEL).reshape(heads, count * rate)
    return full_out, full_level


def combine_levels(branches):
    peak = branches[0][1]
    for entry in branches[1:]:
        peak = jnp.maximum(peak, entry[1])
    numer = jnp.zeros(branches[0][0].shape, jnp.float32)
    denom = jnp.zeros(peak.shape, jnp.float32)
    for entry in branches:
        weight = jnp.exp(entry[1] - peak)
        numer = numer + weight[..., None] * entry[0].astype(jnp.float32)
        denom = denom + weight
    return numer / denom[..., None]


def segment_tokens(query, keys, values, seg_len):
    heads, length, depth = query.shape
    count = length // seg_len

    def split(array):
        return array.reshape(heads, count, seg_len, depth).transpose(1, 0, 2, 3)

    mixed, level = lax.map(lambda triple: attend_per_head(triple[0], triple[1], triple[2]), (split(query), split(keys), split(values)))
    return mixed.transpose(1, 0, 2, 3).reshape(heads, length, depth), level.transpose(1, 0, 2).reshape(heads, length)


def reference(queries, keys, values):
    query_per_head = to_heads(queries)
    key_per_head = to_heads(keys)
    value_per_head = to_heads(values)
    local_output, local_level = segment_tokens(query_per_head, key_per_head, value_per_head, 2 * TOK_DEV)
    central_output, central_level = segment_tokens(dilate_tokens(query_per_head, MIDDLE_DILATION), dilate_tokens(key_per_head, MIDDLE_DILATION), dilate_tokens(value_per_head, MIDDLE_DILATION), MIDDLE_SEGMENT // MIDDLE_DILATION)
    distant_output, distant_level = attend_per_head(dilate_tokens(query_per_head, OUTER_DILATION), dilate_tokens(key_per_head, OUTER_DILATION), dilate_tokens(value_per_head, OUTER_DILATION))
    merged_output = combine_levels([(local_output, local_level), spread_back(central_output, central_level, MIDDLE_DILATION), spread_back(distant_output, distant_level, OUTER_DILATION)])
    far_rows = distant_output.transpose(1, 0, 2).reshape(TOKENS // OUTER_DILATION, H * HD)
    return merged_output.transpose(1, 0, 2).reshape(TOKENS, H * HD).astype(jnp.bfloat16), far_rows
```

```python
import functools

import jax
import jax.numpy as jnp
import numpy as np
from jax import lax
from jax.experimental import pallas as pl
from jax.experimental.pallas import tpu as pltpu
from jax.sharding import PartitionSpec as P


F32 = jnp.float32
BF = jnp.bfloat16
SCALE = float(np.log2(np.e) / 8.0)
PAIRS = 8
TOK = 1024
MID = 256
FAR = 32
CHUNKS = ((0, 2), (2, 2), (4, 2), (6, 1), (7, 1))
RET = 160
VMEM = 56 * 2**20


def params(axes):
    return pltpu.CompilerParams(dimension_semantics=("arbitrary",) * axes, vmem_limit_bytes=VMEM)


def token_class(slot, head):
    a, b = slot // 8, slot % 8
    return 4 * ((b + head // 4) % 8) + (a + head) % 4


def order_matrix(by_class):
    a = lax.broadcasted_iota(jnp.int32, (256, 256), 0)
    b = lax.broadcasted_iota(jnp.int32, (256, 256), 1)
    if not by_class:
        a, b = b, a
    return (b == 32 * (a % 8) + a // 8).astype(F32).astype(BF)


def prep_kernel(q_ref, k_ref, v_ref, qf_ref, qkvm_ref, kvm_ref, kvr_ref, *rest):
    sent, wide = rest[:-1], rest[-1]
    step = pl.program_id(0)
    order = order_matrix(True)
    low = lax.broadcasted_iota(jnp.int32, (8, 128), 1) < 64
    for n, ref in enumerate((q_ref, k_ref, v_ref)):
        for t in range(4):
            block = ref[t * 256 : (t + 1) * 256, :]
            wide[n, t] = jnp.dot(order, block, preferred_element_type=F32)
    for pair in range(2):
        g = 2 * step + pair
        lanes = slice(pair * 128, (pair + 1) * 128)
        for slot in range(32):
            c0 = pl.multiple_of(token_class(slot, 2 * g) * 8, 8)
            c1 = pl.multiple_of(token_class(slot, 2 * g + 1) * 8, 8)
            row = slot * FAR
            for n in range(3):
                x = jnp.concatenate(
                    [
                        jnp.where(low, wide[n, t, pl.ds(c0, 8), lanes], wide[n, t, pl.ds(c1, 8), lanes])
                        for t in range(4)
                    ],
                    axis=0,
                ).astype(BF)
                if n == 0:
                    qf_ref[pair, row : row + FAR, :] = x
                elif slot < 8:
                    kvm_ref[pair, n - 1, row : row + FAR, :] = x
                else:
                    kvr_ref[pair, n - 1, row - MID : row - MID + FAR, :] = x
                if slot < 8:
                    qkvm_ref[pair, n, row : row + FAR, :] = x
    for (first, count), out in zip(CHUNKS, sent):

        @pl.when(step == first // 2)
        def _():
            out[...] = kvr_ref[first % 2 : first % 2 + count]


def prep(q, k, v):
    col = pl.BlockSpec((TOK, 256), lambda g: (0, g))
    return pl.pallas_call(
        prep_kernel,
        grid=(PAIRS // 2,),
        in_specs=[col, col, col],
        out_specs=[
            pl.BlockSpec((2, TOK, 128), lambda g: (g, 0, 0)),
            pl.BlockSpec((2, 3, MID, 128), lambda g: (g, 0, 0, 0)),
            pl.BlockSpec((2, 2, MID, 128), lambda g: (g, 0, 0, 0)),
            pl.BlockSpec((2, 2, TOK - MID, 128), lambda g: (g, 0, 0, 0)),
        ]
        + [pl.BlockSpec((n, 2, TOK - MID, 128), lambda g: (0, 0, 0, 0)) for _, n in CHUNKS],
        out_shape=[
            jax.ShapeDtypeStruct((PAIRS, TOK, 128), BF),
            jax.ShapeDtypeStruct((PAIRS, 3, MID, 128), BF),
            jax.ShapeDtypeStruct((PAIRS, 2, MID, 128), BF),
            jax.ShapeDtypeStruct((PAIRS, 2, TOK - MID, 128), BF),
        ]
        + [jax.ShapeDtypeStruct((n, 2, TOK - MID, 128), BF) for _, n in CHUNKS],
        scratch_shapes=[pltpu.VMEM((3, 4, 256, 256), F32)],
        compiler_params=params(1),
        name="prep",
    )(q, k, v)


def rows_of(refs):
    parts = [r[...].reshape(-1, 128) for r in refs]
    return parts[0] if len(parts) == 1 else jnp.concatenate(parts, axis=0)


def scaled_query(q, head):
    lane = lax.broadcasted_iota(jnp.int32, q.shape, 1)
    own = (lane >= 64) == (head == 1)
    q = q.astype(F32) * SCALE
    hi = q.astype(BF)
    lo = (q - hi.astype(F32)).astype(BF)
    zero = jnp.zeros_like(hi)
    return jnp.concatenate([jnp.where(own, hi, zero), jnp.where(own, lo, zero)], axis=1)


def score(keys, query):
    both = jnp.concatenate([keys, keys], axis=1)
    return lax.dot_general(both, query, (((1,), (1,)), ((), ())), preferred_element_type=F32)


def set_values(vt, v):
    t = v.T
    for e in range(2):
        vt[e, 0:64, :] = t[e * 64 : (e + 1) * 64, :]
        vt[e, 64:80, :] = jnp.ones((16, t.shape[1]), BF)


def mix(vt, p):
    return lax.dot_general(vt, p, (((1,), (0,)), ((), ())), preferred_element_type=F32)


def attend_kernel(*refs, parts, carried, qb, qt):
    q_ref, refs = refs[0], refs[1:]
    k_refs, v_refs, refs = refs[:parts], refs[parts : 2 * parts], refs[2 * parts :]
    if carried:
        oi_ref, mi_ref, refs = refs[0], refs[1], refs[2:]
    o_ref, m_ref, vt = refs

    @pl.when(pl.program_id(1) == 0)
    def _():
        set_values(vt, rows_of(v_refs))

    queries = q_ref[...].reshape(qb, 128)
    keys = rows_of(k_refs)
    safe = jnp.ones((1, qt), F32)
    for t in range(qb // qt):
        cols = slice(t * qt, (t + 1) * qt)
        for e in range(2):
            s = score(keys, scaled_query(queries[t * qt : (t + 1) * qt], e))
            a = mix(vt[e], jnp.exp2(s).astype(BF))
            o, den = a[:64], a[64:65]
            if carried:
                o = o + oi_ref[0, e * 64 : (e + 1) * 64, cols]
                den = den + mi_ref[0, 2 * e + 1, :, cols]
                safe = jnp.where(mi_ref[0, 2 * e, :, cols] == 0.0, safe, 0.0)
            safe = jnp.where((den > 2.0**-80) & (den < 2.0**120), safe, 0.0)
            o_ref[0, e * 64 : (e + 1) * 64, cols] = o
            m_ref[0, 2 * e, :, cols] = jnp.zeros((1, qt), F32)
            m_ref[0, 2 * e + 1, :, cols] = den

    @pl.when(jnp.min(safe) < 0.5)
    def _():
        def shifted(n, carry):
            e = n % 2
            cols = pl.ds(pl.multiple_of((n // 2) * 256, 256), 256)
            heads = pl.ds(pl.multiple_of(e * 64, 64), 64)
            if len(q_ref.shape) == 3:
                q = q_ref[0, cols, :]
            else:
                q = q_ref[n // 2, 0]
            s = score(rows_of(k_refs), scaled_query(q, e))
            peak = jnp.max(s, axis=0, keepdims=True)
            if carried:
                peak = jnp.maximum(peak, mi_ref[0, 2 * e, :, cols])
            a = mix(vt[e], jnp.exp2(s - peak).astype(BF))
            o, den = a[:64], a[64:65]
            if carried:
                w = jnp.exp2(mi_ref[0, 2 * e, :, cols] - peak)
                o = o + w * oi_ref[0, heads, cols]
                den = den + w * mi_ref[0, 2 * e + 1, :, cols]
            o_ref[0, heads, cols] = o
            m_ref[0, 2 * e, :, cols] = peak
            m_ref[0, 2 * e + 1, :, cols] = den
            return carry

        lax.fori_loop(0, 2 * (qb // 256), shifted, 0)


def attend(groups, nq, qb, qt, query, parts, carry=None, carry_first=0):
    nk = sum(p[3] for p in parts)
    specs = [query[1]] + [p[1] for p in parts] + [p[2] for p in parts]
    args = [query[0]] + [p[0] for p in parts] + [p[0] for p in parts]

    def carry_specs(first):
        return [
            pl.BlockSpec((1, 128, qb), lambda g, j: (g + first, 0, j)),
            pl.BlockSpec((1, 4, 1, qb), lambda g, j: (g + first, 0, 0, j)),
        ]

    if carry is not None:
        specs += carry_specs(carry_first)
        args += list(carry)
    exps = groups * 2 * nq * nk
    return pl.pallas_call(
        functools.partial(
            attend_kernel, parts=len(parts), carried=carry is not None, qb=qb, qt=qt
        ),
        grid=(groups, nq // qb),
        in_specs=specs,
        out_specs=carry_specs(0),
        out_shape=[
            jax.ShapeDtypeStruct((groups, 128, nq), F32),
            jax.ShapeDtypeStruct((groups, 4, 1, nq), F32),
        ],
        scratch_shapes=[pltpu.VMEM((2, 80, nk), BF)],
        compiler_params=params(2),
        cost_estimate=pl.CostEstimate(
            flops=exps * 1100, bytes_accessed=groups * (nq + nk) * 1024, transcendentals=exps
        ),
    )(*args)


def near(first, count, qf, kvm, kvr, kvr_first, carry=None, carry_first=0):
    def part(array, base, rows):
        return (
            array,
            pl.BlockSpec((1, 1, rows, 128), lambda g, j: (g + base, 0, 0, 0)),
            pl.BlockSpec((1, 1, rows, 128), lambda g, j: (g + base, 1, 0, 0)),
            rows,
        )

    return attend(
        count,
        TOK,
        TOK,
        1024,
        (qf, pl.BlockSpec((1, TOK, 128), lambda g, j: (g + first, j, 0))),
        [part(kvm, first, MID), part(kvr, kvr_first, TOK - MID)],
        carry,
        carry_first,
    )


def middle(own, keys, at, carry=None):
    nq = PAIRS * MID
    qb = 1024
    return attend(
        1,
        nq,
        qb,
        512,
        (own, pl.BlockSpec((qb // MID, 1, MID, 128), lambda g, j: (j, 0, 0, 0))),
        [
            (
                keys,
                pl.BlockSpec((PAIRS, 1, MID, 128), lambda g, j: (0, at, 0, 0)),
                pl.BlockSpec((PAIRS, 1, MID, 128), lambda g, j: (0, at + 1, 0, 0)),
                PAIRS * MID,
            )
        ],
        carry,
    )


def far_kernel(q_ref, ka, kb, kc, va, vb, vc, o_ref, m_ref, ret_ref, vt):
    set_values(vt, rows_of((va, vb, vc)))
    keys = rows_of((ka, kb, kc))
    queries = rows_of((q_ref,))
    outs, levels = [], []
    for e in range(2):
        s = score(keys, scaled_query(queries, e))
        peak = jnp.max(s, axis=0, keepdims=True)
        a = mix(vt[e], jnp.exp2(s - peak).astype(BF))
        outs.append(a[:64] / a[64:65])
        levels.append(peak + jnp.log2(a[64:65]))
    row = lax.broadcasted_iota(jnp.int32, (16, MID), 0)
    first = lax.broadcasted_iota(jnp.int32, (1, MID), 1) < FAR
    for d in range(PAIRS):
        cols = slice(d * MID, (d + 1) * MID)
        lev = jnp.zeros((16, MID), F32)
        for e in range(2):
            heads = slice(e * 64, (e + 1) * 64)
            peak = m_ref[0, 2 * e, :, cols]
            den = m_ref[0, 2 * e + 1, :, cols]
            o = o_ref[0, heads, cols]
            fo = outs[e][:, d * FAR : (d + 1) * FAR]
            fl = levels[e][:, d * FAR : (d + 1) * FAR]
            fo = jnp.concatenate([fo, jnp.zeros((64, MID - FAR), F32)], axis=1)
            fl = jnp.concatenate([fl, jnp.zeros((1, MID - FAR), F32)], axis=1)
            fl = jnp.where(first, fl, -1e30)
            top = jnp.maximum(peak, fl)
            wm = jnp.exp2(peak - top)
            wf = jnp.exp2(fl - top)
            total = wm * den + wf
            ret_ref[d, heads, :] = ((wm * o + wf * fo) / total).astype(BF)
            level = top + jnp.log2(total)
            for part in range(3):
                piece = level.astype(BF).astype(F32)
                level = level - piece
                lev = jnp.where(row == 3 * e + part, piece, lev)
        ret_ref[d, 128:144, :] = lev.astype(BF)
        ret_ref[d, 144:160, :] = jnp.concatenate(
            [
                outs[b // 4][16 * (b % 4) : 16 * (b % 4) + 16, d * FAR : (d + 1) * FAR]
                for b in range(8)
            ],
            axis=1,
        ).astype(BF)


def far_and_return(own, partner, other, mid):
    def part(lead, at):
        return pl.BlockSpec((lead, 1, FAR, 128), lambda i: (0, at, 0, 0))

    whole = lambda i: (0, 0, 0)
    return pl.pallas_call(
        far_kernel,
        grid=(1,),
        in_specs=[
            part(PAIRS, 0),
            part(PAIRS, 1),
            part(PAIRS, 0),
            part(2 * PAIRS, 0),
            part(PAIRS, 2),
            part(PAIRS, 1),
            part(2 * PAIRS, 1),
            pl.BlockSpec((1, 128, PAIRS * MID), whole),
            pl.BlockSpec((1, 4, 1, PAIRS * MID), lambda i: (0, 0, 0, 0)),
        ],
        out_specs=pl.BlockSpec((PAIRS, RET, MID), whole),
        out_shape=jax.ShapeDtypeStruct((PAIRS, RET, MID), BF),
        scratch_shapes=[pltpu.VMEM((2, 80, 1024), BF)],
        compiler_params=params(1),
        name="far",
    )(own, own, partner, other, own, partner, other, *mid)


def merge_kernel(o_ref, m_ref, ret_ref, *rest, first):
    out_ref, turned = rest[-2:]
    g = pl.program_id(0) + first
    parts = []
    lev = ret_ref[0, 128:144, :].astype(F32)
    for e in range(2):
        heads = slice(e * 64, (e + 1) * 64)
        peak = m_ref[0, 2 * e, :, :MID]
        den = m_ref[0, 2 * e + 1, :, :MID]
        level = lev[3 * e : 3 * e + 1] + lev[3 * e + 1 : 3 * e + 2] + lev[3 * e + 2 : 3 * e + 3]
        top = jnp.maximum(peak, level)
        wn = jnp.exp2(peak - top)
        wm = jnp.exp2(level - top)
        inv = 1.0 / (wn * den + wm)
        head = (wn * inv) * o_ref[0, heads, :MID] + (wm * inv) * ret_ref[0, heads, :].astype(F32)
        tail = o_ref[0, heads, MID:] * (1.0 / m_ref[0, 2 * e + 1, :, MID:])
        parts.append(jnp.concatenate([head, tail], axis=1))
    turned[...] = jnp.concatenate(parts, axis=0).T
    order = order_matrix(False)
    low = lax.broadcasted_iota(jnp.int32, (8, 128), 1) < 64
    starts = []
    for cls in range(32):
        for e in range(2):
            h = 2 * g + e
            a = (cls % 4 - h + 16) % 4
            b = (cls // 4 - h // 4 + 8) % 8
            starts.append(a * 256 + b * 32)
    for t in range(4):
        rows = []
        for cls in range(32):
            r0 = pl.multiple_of(starts[2 * cls] + 8 * t, 8)
            r1 = pl.multiple_of(starts[2 * cls + 1] + 8 * t, 8)
            rows.append(jnp.where(low, turned[pl.ds(r0, 8), :], turned[pl.ds(r1, 8), :]))
        block = jnp.concatenate(rows, axis=0).astype(BF)
        out_ref[t * 256 : (t + 1) * 256, :] = jnp.dot(
            order, block, preferred_element_type=F32
        ).astype(BF)


def merge(first, count, carry, ret, out):
    specs = [
        pl.BlockSpec((1, 128, TOK), lambda g: (g, 0, 0)),
        pl.BlockSpec((1, 4, 1, TOK), lambda g: (g, 0, 0, 0)),
        pl.BlockSpec((1, RET, MID), lambda g: (g + first, 0, 0)),
    ]
    args = [*carry, ret]
    alias = {}
    if out is not None:
        specs.append(pl.BlockSpec(memory_space=pl.ANY))
        args.append(out)
        alias = {3: 0}
    return pl.pallas_call(
        functools.partial(merge_kernel, first=first),
        grid=(count,),
        in_specs=specs,
        out_specs=pl.BlockSpec((TOK, 128), lambda g: (0, g + first)),
        out_shape=jax.ShapeDtypeStruct((TOK, PAIRS * 128), BF),
        scratch_shapes=[pltpu.VMEM((TOK, 128), F32)],
        input_output_aliases=alias,
        compiler_params=params(1),
        name="merge",
    )(*args)


GROUPS = [
    [y * 16 + x * 4 + z for x in range(4) for z in pair] for y in range(2) for pair in ((1, 2), (0, 3))
]
NEAR = [(i, i ^ 1) for i in range(32)]
PLANE = [(i, i ^ 16) for i in range(32)]


def exchange(x):
    return lax.all_to_all(x, "seq", 0, 0, axis_index_groups=GROUPS, tiled=True)


def steps(queries, keys, values):
    qf, qkvm, kvm, kvr, *sent = prep(queries, keys, values)
    kvm_there = lax.ppermute(kvm, "seq", NEAR)
    own = exchange(qkvm)
    kvr_there = []
    for part in sent:
        kvr_there.append(lax.ppermute(part, "seq", NEAR))
    partner = exchange(kvm_there)
    half = PAIRS // 2
    here = []
    for i in range(2):
        here.append(near(i * half, half, qf, kvm, kvr, i * half))
    far_kv = jnp.concatenate([own[:, 1:, :FAR], partner[:, :, :FAR]], axis=0)
    other = lax.ppermute(far_kv, "seq", PLANE)
    mid = middle(own, own, 1)
    mid = middle(own, partner, 0, mid)
    ret = far_and_return(own, partner, other, mid)
    ret = exchange(ret)
    far_rows = ret[:, 144:, :].reshape(PAIRS, 16, 8, FAR).transpose(3, 0, 2, 1).reshape(FAR, PAIRS * 128)
    out = None
    for i, (a, n) in enumerate(CHUNKS):
        both = near(a, n, qf, kvm_there, kvr_there[i], 0, here[a // half], a % half)
        out = merge(a, n, both, ret, out)
    return out, far_rows


def solution(mesh):
    spec = P(("dp", "seq"), None)
    return jax.shard_map(
        steps, mesh=mesh, in_specs=(spec, spec, spec), out_specs=(spec, spec), check_vma=False
    )
```

```python
import functools

import jax
import jax.numpy as jnp
import numpy as np
from jax import lax
from jax.experimental import pallas as pl
from jax.experimental.pallas import tpu as pltpu
from jax.sharding import PartitionSpec as P


F32 = jnp.float32
BF = jnp.bfloat16
SCALE = float(np.log2(np.e) / 8.0)
PAIRS = 8
TOK = 1024
MID = 256
FAR = 32
CHUNKS = ((0, 2), (2, 3), (5, 2), (7, 1))
RET = 176
WIDE = 56 * 2**20
SLIM = 30 * 2**20


def params(axes, limit=WIDE):
    return pltpu.CompilerParams(dimension_semantics=("arbitrary",) * axes, vmem_limit_bytes=limit)


def token_class(slot, head):
    a, b = slot // 8, slot % 8
    return 4 * ((b + head // 4) % 8) + (a + head) % 4


def order_matrix(by_class):
    a = lax.broadcasted_iota(jnp.int32, (256, 256), 0)
    b = lax.broadcasted_iota(jnp.int32, (256, 256), 1)
    if not by_class:
        a, b = b, a
    return (b == 32 * (a % 8) + a // 8).astype(F32).astype(BF)


def prep_kernel(q_ref, k_ref, v_ref, *outs):
    for step in range(PAIRS // 2):

        @pl.when(pl.program_id(0) == step)
        def _():
            prep_step(step, (q_ref, k_ref, v_ref), *outs)


def prep_step(step, refs, qf_ref, qkvm_ref, kvm_ref, *sent):
    order = order_matrix(True)
    low = lax.broadcasted_iota(jnp.int32, (8, 128), 1) < 64
    for n, ref in enumerate(refs):
        blocks = [
            jnp.dot(order, ref[t * 256 : (t + 1) * 256, :], preferred_element_type=F32)
            for t in range(4)
        ]
        for pair in range(2):
            g = 2 * step + pair
            chunk = [c for c, (first, count) in enumerate(CHUNKS) if first <= g < first + count][0]
            at = g - CHUNKS[chunk][0]
            lanes = slice(pair * 128, (pair + 1) * 128)
            for slot in range(32):
                c0 = token_class(slot, 2 * g) * 8
                c1 = token_class(slot, 2 * g + 1) * 8
                x = jnp.concatenate(
                    [
                        jnp.where(low, y[c0 : c0 + 8, lanes], y[c1 : c1 + 8, lanes])
                        for y in blocks
                    ],
                    axis=0,
                ).astype(BF)
                row = slot * FAR
                if n == 0:
                    qf_ref[pair, row : row + FAR, :] = x
                elif slot < 8:
                    kvm_ref[pair, n - 1, row : row + FAR, :] = x
                else:
                    sent[chunk][at, n - 1, row - MID : row - MID + FAR, :] = x
                if slot < 8:
                    qkvm_ref[pair, n, row : row + FAR, :] = x


def prep(q, k, v):
    col = pl.BlockSpec((TOK, 256), lambda g: (0, g))
    return pl.pallas_call(
        prep_kernel,
        grid=(PAIRS // 2,),
        in_specs=[col, col, col],
        out_specs=[
            pl.BlockSpec((2, TOK, 128), lambda g: (g, 0, 0)),
            pl.BlockSpec((2, 3, MID, 128), lambda g: (g, 0, 0, 0)),
            pl.BlockSpec((2, 2, MID, 128), lambda g: (g, 0, 0, 0)),
        ]
        + [pl.BlockSpec((n, 2, TOK - MID, 128), lambda g: (0, 0, 0, 0)) for _, n in CHUNKS],
        out_shape=[
            jax.ShapeDtypeStruct((PAIRS, TOK, 128), BF),
            jax.ShapeDtypeStruct((PAIRS, 3, MID, 128), BF),
            jax.ShapeDtypeStruct((PAIRS, 2, MID, 128), BF),
        ]
        + [jax.ShapeDtypeStruct((n, 2, TOK - MID, 128), BF) for _, n in CHUNKS],
        compiler_params=params(1),
        name="prep",
    )(q, k, v)


def rows_of(refs):
    parts = [r[...].reshape(-1, 128) for r in refs]
    return parts[0] if len(parts) == 1 else jnp.concatenate(parts, axis=0)


def scaled_query(q, head):
    lane = lax.broadcasted_iota(jnp.int32, q.shape, 1)
    own = (lane >= 64) == (head == 1)
    q = q.astype(F32) * SCALE
    hi = q.astype(BF)
    lo = (q - hi.astype(F32)).astype(BF)
    zero = jnp.zeros_like(hi)
    return jnp.concatenate([jnp.where(own, hi, zero), jnp.where(own, lo, zero)], axis=1)


def score(keys, query):
    both = jnp.concatenate([keys, keys], axis=1)
    return lax.dot_general(both, query, (((1,), (1,)), ((), ())), preferred_element_type=F32)


def set_values(vt, v):
    t = v.T
    for e in range(2):
        vt[e, 0:64, :] = t[e * 64 : (e + 1) * 64, :]
        vt[e, 64:80, :] = jnp.ones((16, t.shape[1]), BF)


def mix(vt, p):
    return lax.dot_general(vt, p, (((1,), (0,)), ((), ())), preferred_element_type=F32)


def attend_kernel(*refs, parts, carried, qb, qt):
    q_ref, refs = refs[0], refs[1:]
    k_refs, v_refs, refs = refs[:parts], refs[parts : 2 * parts], refs[2 * parts :]
    carry = None
    if carried:
        carry, refs = refs[:2], refs[2:]
    attend_body(q_ref, k_refs, v_refs, carry, *refs, qb, qt)


def attend_body(q_ref, k_refs, v_refs, carry, o_ref, m_ref, vt, qb, qt):
    carried = carry is not None
    if carried:
        oi_ref, mi_ref = carry

    @pl.when(pl.program_id(1) == 0)
    def _():
        set_values(vt, rows_of(v_refs))

    queries = q_ref[...].reshape(qb, 128)
    keys = rows_of(k_refs)
    safe = jnp.ones((1, qt), F32)
    for t in range(qb // qt):
        cols = slice(t * qt, (t + 1) * qt)
        for e in range(2):
            s = score(keys, scaled_query(queries[t * qt : (t + 1) * qt], e))
            a = mix(vt[e], jnp.exp2(s).astype(BF))
            o, den = a[:64], a[64:65]
            if carried:
                o = o + oi_ref[0, e * 64 : (e + 1) * 64, cols]
                den = den + mi_ref[0, 2 * e + 1, :, cols]
                safe = jnp.where(mi_ref[0, 2 * e, :, cols] == 0.0, safe, 0.0)
            safe = jnp.where((den > 2.0**-80) & (den < 2.0**120), safe, 0.0)
            o_ref[0, e * 64 : (e + 1) * 64, cols] = o
            m_ref[0, 2 * e, :, cols] = jnp.zeros((1, qt), F32)
            m_ref[0, 2 * e + 1, :, cols] = den

    @pl.when(jnp.min(safe) < 0.5)
    def _():
        def shifted(n, state):
            e = n % 2
            cols = pl.ds(pl.multiple_of((n // 2) * 256, 256), 256)
            heads = pl.ds(pl.multiple_of(e * 64, 64), 64)
            if len(q_ref.shape) == 3:
                q = q_ref[0, cols, :]
            else:
                q = q_ref[n // 2, 0]
            s = score(rows_of(k_refs), scaled_query(q, e))
            peak = jnp.max(s, axis=0, keepdims=True)
            if carried:
                peak = jnp.maximum(peak, mi_ref[0, 2 * e, :, cols])
            a = mix(vt[e], jnp.exp2(s - peak).astype(BF))
            o, den = a[:64], a[64:65]
            if carried:
                w = jnp.exp2(mi_ref[0, 2 * e, :, cols] - peak)
                o = o + w * oi_ref[0, heads, cols]
                den = den + w * mi_ref[0, 2 * e + 1, :, cols]
            o_ref[0, heads, cols] = o
            m_ref[0, 2 * e, :, cols] = peak
            m_ref[0, 2 * e + 1, :, cols] = den
            return state

        lax.fori_loop(0, 2 * (qb // 256), shifted, 0)


def carry_specs(first, qb):
    return [
        pl.BlockSpec((1, 128, qb), lambda g, j: (g + first, 0, j)),
        pl.BlockSpec((1, 4, 1, qb), lambda g, j: (g + first, 0, 0, j)),
    ]


def attend(groups, nq, qb, qt, query, parts, carry=None, first=None, limit=WIDE):
    nk = sum(p[3] for p in parts)
    specs = [query[1]] + [p[1] for p in parts] + [p[2] for p in parts]
    args = [query[0]] + [p[0] for p in parts] + [p[4] if len(p) > 4 else p[0] for p in parts]

    alias = {}
    if first is not None:
        alias = {len(args): 0, len(args) + 1: 1}
    if carry is not None:
        specs += carry_specs(first or 0, qb)
        args += list(carry)
    total = groups if first is None else carry[0].shape[0]
    exps = groups * 2 * nq * nk
    return pl.pallas_call(
        functools.partial(
            attend_kernel, parts=len(parts), carried=carry is not None, qb=qb, qt=qt
        ),
        grid=(groups, nq // qb),
        in_specs=specs,
        out_specs=carry_specs(first or 0, qb),
        out_shape=[
            jax.ShapeDtypeStruct((total, 128, nq), F32),
            jax.ShapeDtypeStruct((total, 4, 1, nq), F32),
        ],
        scratch_shapes=[pltpu.VMEM((2, 80, nk), BF)],
        input_output_aliases=alias,
        compiler_params=params(2, limit),
        cost_estimate=pl.CostEstimate(
            flops=exps * 1100, bytes_accessed=groups * (nq + nk) * 1024, transcendentals=exps
        ),
    )(*args)


def near_part(array, base, rows):
    return (
        array,
        pl.BlockSpec((1, 1, rows, 128), lambda g, j: (g + base, 0, 0, 0)),
        pl.BlockSpec((1, 1, rows, 128), lambda g, j: (g + base, 1, 0, 0)),
        rows,
    )


def near_query(qf, first):
    return (qf, pl.BlockSpec((1, TOK, 128), lambda g, j: (g + first, j, 0)))


def near_here(first, count, qf, keys, values):
    col = pl.BlockSpec((TOK, 128), lambda g, j: (0, g + first))
    part = (keys, col, col, TOK, values)
    return attend(count, TOK, TOK, 1024, near_query(qf, first), [part])


def near_there(first, count, qf, kvm, kvr, carry):
    parts = [near_part(kvm, first, MID), near_part(kvr, 0, TOK - MID)]
    return attend(count, TOK, TOK, 1024, near_query(qf, first), parts, carry, first)


def middle(own, keys, at, carry=None):
    nq = PAIRS * MID
    qb = 1024
    return attend(
        1,
        nq,
        qb,
        512,
        (own, pl.BlockSpec((qb // MID, 1, MID, 128), lambda g, j: (j, 0, 0, 0))),
        [
            (
                keys,
                pl.BlockSpec((PAIRS, 1, MID, 128), lambda g, j: (0, at, 0, 0)),
                pl.BlockSpec((PAIRS, 1, MID, 128), lambda g, j: (0, at + 1, 0, 0)),
                PAIRS * MID,
            )
        ],
        carry,
        limit=SLIM,
    )


def far_kernel(q_ref, ka, kb, kc, va, vb, vc, o_ref, m_ref, ret_ref, vt):
    set_values(vt, rows_of((va, vb, vc)))
    keys = rows_of((ka, kb, kc))
    queries = rows_of((q_ref,))
    outs, levels = [], []
    for e in range(2):
        s = score(keys, scaled_query(queries, e))
        peak = jnp.max(s, axis=0, keepdims=True)
        a = mix(vt[e], jnp.exp2(s - peak).astype(BF))
        outs.append(a[:64] / a[64:65])
        levels.append(peak + jnp.log2(a[64:65]))
    far = jnp.concatenate(outs, axis=0).T
    row = lax.broadcasted_iota(jnp.int32, (16, MID), 0)
    first = lax.broadcasted_iota(jnp.int32, (1, MID), 1) < FAR
    for d in range(PAIRS):
        cols = slice(d * MID, (d + 1) * MID)
        lev = jnp.zeros((16, MID), F32)
        for e in range(2):
            heads = slice(e * 64, (e + 1) * 64)
            peak = m_ref[0, 2 * e, :, cols]
            den = m_ref[0, 2 * e + 1, :, cols]
            o = o_ref[0, heads, cols]
            fo = outs[e][:, d * FAR : (d + 1) * FAR]
            fl = levels[e][:, d * FAR : (d + 1) * FAR]
            fo = jnp.concatenate([fo, jnp.zeros((64, MID - FAR), F32)], axis=1)
            fl = jnp.concatenate([fl, jnp.zeros((1, MID - FAR), F32)], axis=1)
            fl = jnp.where(first, fl, -1e30)
            top = jnp.maximum(peak, fl)
            wm = jnp.exp2(peak - top)
            wf = jnp.exp2(fl - top)
            total = wm * den + wf
            ret_ref[d, heads, :] = ((wm * o + wf * fo) / total).astype(BF)
            level = top + jnp.log2(total)
            for part in range(3):
                piece = level.astype(BF).astype(F32)
                level = level - piece
                lev = jnp.where(row == 3 * e + part, piece, lev)
        ret_ref[d, 128:144, :] = lev.astype(BF)
        ret_ref[d, 144:176, 0:128] = far[d * FAR : (d + 1) * FAR].astype(BF)
        ret_ref[d, 144:176, 128:256] = jnp.zeros((FAR, 128), BF)


def far_and_return(own, partner, other, mid):
    def part(lead, at):
        return pl.BlockSpec((lead, 1, FAR, 128), lambda i: (0, at, 0, 0))

    whole = lambda i: (0, 0, 0)
    return pl.pallas_call(
        far_kernel,
        grid=(1,),
        in_specs=[
            part(PAIRS, 0),
            part(PAIRS, 1),
            part(PAIRS, 0),
            part(2 * PAIRS, 0),
            part(PAIRS, 2),
            part(PAIRS, 1),
            part(2 * PAIRS, 1),
            pl.BlockSpec((1, 128, PAIRS * MID), whole),
            pl.BlockSpec((1, 4, 1, PAIRS * MID), lambda i: (0, 0, 0, 0)),
        ],
        out_specs=pl.BlockSpec((PAIRS, RET, MID), whole),
        out_shape=jax.ShapeDtypeStruct((PAIRS, RET, MID), BF),
        scratch_shapes=[pltpu.VMEM((2, 80, 1024), BF)],
        compiler_params=params(1, SLIM),
        name="far",
    )(own, own, partner, other, own, partner, other, *mid)


def merge_kernel(o_ref, m_ref, ret_ref, *rest, first):
    merge_body(o_ref, m_ref, ret_ref, *rest[-2:], pl.program_id(0) + first)


def finish_kernel(q_ref, ka, kb, va, vb, oi_ref, mi_ref, ret_ref, *rest, first):
    out_ref, vt, o_ref, m_ref, turned = rest[-5:]
    attend_body(q_ref, (ka, kb), (va, vb), (oi_ref, mi_ref), o_ref, m_ref, vt, TOK, 1024)
    merge_body(o_ref, m_ref, ret_ref, out_ref, turned, pl.program_id(0) + first)


def merge_body(o_ref, m_ref, ret_ref, out_ref, turned, g):
    parts = []
    lev = ret_ref[0, 128:144, :].astype(F32)
    for e in range(2):
        heads = slice(e * 64, (e + 1) * 64)
        peak = m_ref[0, 2 * e, :, :MID]
        den = m_ref[0, 2 * e + 1, :, :MID]
        level = lev[3 * e : 3 * e + 1] + lev[3 * e + 1 : 3 * e + 2] + lev[3 * e + 2 : 3 * e + 3]
        top = jnp.maximum(peak, level)
        wn = jnp.exp2(peak - top)
        wm = jnp.exp2(level - top)
        inv = 1.0 / (wn * den + wm)
        head = (wn * inv) * o_ref[0, heads, :MID] + (wm * inv) * ret_ref[0, heads, :].astype(F32)
        tail = o_ref[0, heads, MID:] * (1.0 / m_ref[0, 2 * e + 1, :, MID:])
        parts.append(jnp.concatenate([head, tail], axis=1))
    turned[...] = jnp.concatenate(parts, axis=0).T
    order = order_matrix(False)
    low = lax.broadcasted_iota(jnp.int32, (8, 128), 1) < 64
    starts = []
    for cls in range(32):
        for e in range(2):
            h = 2 * g + e
            a = (cls % 4 - h + 16) % 4
            b = (cls // 4 - h // 4 + 8) % 8
            starts.append(a * 256 + b * 32)
    for t in range(4):
        rows = []
        for cls in range(32):
            r0 = pl.multiple_of(starts[2 * cls] + 8 * t, 8)
            r1 = pl.multiple_of(starts[2 * cls + 1] + 8 * t, 8)
            rows.append(jnp.where(low, turned[pl.ds(r0, 8), :], turned[pl.ds(r1, 8), :]))
        block = jnp.concatenate(rows, axis=0).astype(BF)
        out_ref[t * 256 : (t + 1) * 256, :] = jnp.dot(
            order, block, preferred_element_type=F32
        ).astype(BF)


def merge(first, count, carry, ret, out):
    specs = [
        pl.BlockSpec((1, 128, TOK), lambda g: (g, 0, 0)),
        pl.BlockSpec((1, 4, 1, TOK), lambda g: (g, 0, 0, 0)),
        pl.BlockSpec((1, RET, MID), lambda g: (g + first, 0, 0)),
    ]
    args = [*carry, ret]
    alias = {}
    if out is not None:
        specs.append(pl.BlockSpec(memory_space=pl.ANY))
        args.append(out)
        alias = {3: 0}
    return pl.pallas_call(
        functools.partial(merge_kernel, first=first),
        grid=(count,),
        in_specs=specs,
        out_specs=pl.BlockSpec((TOK, 128), lambda g: (0, g + first)),
        out_shape=jax.ShapeDtypeStruct((TOK, PAIRS * 128), BF),
        scratch_shapes=[pltpu.VMEM((TOK, 128), F32)],
        input_output_aliases=alias,
        compiler_params=params(1),
        name="merge",
    )(*args)


def finish(first, count, qf, kvm, kvr, carry, carry_first, ret, out):
    query = near_query(qf, first)
    parts = [near_part(kvm, first, MID), near_part(kvr, 0, TOK - MID)]
    specs = [query[1]] + [p[1] for p in parts] + [p[2] for p in parts]
    specs += carry_specs(carry_first, TOK)
    specs += [
        pl.BlockSpec((1, RET, MID), lambda g, j: (g + first, 0, 0)),
        pl.BlockSpec(memory_space=pl.ANY),
    ]
    args = [qf, kvm, kvr, kvm, kvr, *carry, ret, out]
    return pl.pallas_call(
        functools.partial(finish_kernel, first=first),
        grid=(count, 1),
        in_specs=specs,
        out_specs=pl.BlockSpec((TOK, 128), lambda g, j: (0, g + first)),
        out_shape=jax.ShapeDtypeStruct((TOK, PAIRS * 128), BF),
        scratch_shapes=[
            pltpu.VMEM((2, 80, TOK), BF),
            pltpu.VMEM((1, 128, TOK), F32),
            pltpu.VMEM((1, 4, 1, TOK), F32),
            pltpu.VMEM((TOK, 128), F32),
        ],
        input_output_aliases={len(args) - 1: 0},
        compiler_params=params(2),
        name="finish",
    )(*args)


GROUPS = [
    [y * 16 + x * 4 + z for x in range(4) for z in pair] for y in range(2) for pair in ((1, 2), (0, 3))
]
NEAR = [(i, i ^ 1) for i in range(32)]
PLANE = [(i, i ^ 16) for i in range(32)]


def exchange(x):
    return lax.all_to_all(x, "seq", 0, 0, axis_index_groups=GROUPS, tiled=True)


def steps(queries, keys, values):
    qf, qkvm, kvm, *sent = prep(queries, keys, values)
    kvm_there = lax.ppermute(kvm, "seq", NEAR)
    own = exchange(qkvm)
    kvr_there = []
    for part in sent:
        kvr_there.append(lax.ppermute(part, "seq", NEAR))
    partner = exchange(kvm_there)
    near = near_here(0, PAIRS, qf, keys, values)
    far_kv = jnp.concatenate([own[:, 1:, :FAR], partner[:, :, :FAR]], axis=0)
    other = lax.ppermute(far_kv, "seq", PLANE)
    mid = middle(own, own, 1)
    mid = middle(own, partner, 0, mid)
    ret = far_and_return(own, partner, other, mid)
    ret = exchange(ret)
    far_rows = ret[:, 144:, :128].transpose(1, 0, 2).reshape(FAR, PAIRS * 128)
    for i in (0, 1):
        near = near_there(*CHUNKS[i], qf, kvm_there, kvr_there[i], near)
    out = merge(0, CHUNKS[2][0], near, ret, None)
    for i in (2, 3):
        a, n = CHUNKS[i]
        out = finish(a, n, qf, kvm_there, kvr_there[i], near, a, ret, out)
    return out, far_rows


def solution(mesh):
    spec = P(("dp", "seq"), None)
    return jax.shard_map(
        steps, mesh=mesh, in_specs=(spec, spec, spec), out_specs=(spec, spec), check_vma=False
    )
```
